16 devices in a mesh: data: 16 (over z, y, x, core).
Axes of the slice: x: 2, y: 2, z: 2, core: 2. Of those that a mesh axis runs over, the one named last changes fastest.
Arguments:
- x_in: bfloat16 [32768, 768], P('data')
- dy_in: bfloat16 [32768, 768], P('data')
- weights: bfloat16 [4, 768, 768], replicated
- a_old: float32 [3072, 768], P('data')
- s_old: float32 [3072, 768], P('data')
- a_inv: float32 [3072, 768], P('data')
- s_inv: float32 [4, 768, 768], replicated
Outputs:
- output 1: float32 [4, 768, 768], replicated
- output 2: float32 [3072, 768], P('data')
- output 3: float32 [3072, 768], P('data')
All inputs are finite; a program needn't handle non-finite values.
Results may differ from the reference program's by a relative error of at most 0.00184902.
Values are sent between devices in bfloat16 or wider.
A program may use at most 1 GiB of HBM per device.

```python
import functools
import jax
import jax.numpy as jnp

D = 768
LAYERS = 4
TOKENS = 2048
SHARDS = 16
LOW_RANK = 64
BATCH_TOTAL = TOKENS * SHARDS
FACTOR_DECAY = 0.75


def spd_stack(rng_key, base_diag, gram_scale):
    low_rank = jax.random.normal(rng_key, (LAYERS, D, LOW_RANK), jnp.float32)
    gram_mat = jnp.einsum("lir,ljr->lij", low_rank, low_rank)
    gram_mat = 0.5 * (gram_mat + jnp.swapaxes(gram_mat, 1, 2))
    return gram_scale * gram_mat + base_diag * jnp.eye(D, dtype=jnp.float32)


def shard_rows(rng_key, spread):
    key_raw, key_mean, key_scale = jax.random.split(rng_key, 3)
    raw_rows = jax.random.normal(key_raw, (SHARDS, TOKENS, D), jnp.float32)
    offset = 0.7 * jax.random.normal(key_mean, (SHARDS, 1, D), jnp.float32)
    row_scale = jnp.exp(spread * jax.random.normal(key_scale, (SHARDS, 1, 1), jnp.float32))
    return ((raw_rows + offset) * row_scale).reshape(BATCH_TOTAL, D).astype(jnp.bfloat16)


def setup_inputs(seed: int = 0) -> dict:
    key_list = jax.random.split(jax.random.key(seed), 7)
    weights = jax.random.normal(key_list[2], (LAYERS, D, D), jnp.float32) * D ** -0.5
    inv_scale = (LOW_RANK * D) ** -0.5
    return {
        "x_in": shard_rows(key_list[0], 0.5),
        "dy_in": shard_rows(key_list[1], 0.5),
        "weights": weights.astype(jnp.bfloat16),
        "a_old": spd_stack(key_list[3], 0.5, 1.0 / LOW_RANK).reshape(LAYERS * D, D),
        "s_old": spd_stack(key_list[4], 0.5, 1.0 / LOW_RANK).reshape(LAYERS * D, D),
        "a_inv": spd_stack(key_list[5], 0.5, inv_scale).reshape(LAYERS * D, D),
        "s_inv": spd_stack(key_list[6], 0.5, inv_scale),
    }


def gelu_grad(pre_act, d_act):
    pullback = jax.vjp(functools.partial(jax.nn.gelu, approximate=True), pre_act.astype(jnp.float32))[1]
    return pullback(d_act.astype(jnp.float32))[0].astype(jnp.bfloat16)


def reference(x_in, dy_in, weights, a_old, s_old, a_inv, s_inv):
    layer_inputs = [x_in]
    pre_acts = []
    for layer_id in range(LAYERS - 1):
        pre_act = jnp.dot(layer_inputs[layer_id], weights[layer_id], preferred_element_type=jnp.float32).astype(jnp.bfloat16)
        pre_acts.append(pre_act)
        layer_inputs.append(jax.nn.gelu(pre_act.astype(jnp.float32), approximate=True).astype(jnp.bfloat16))
    out_grads = [dy_in] * LAYERS
    for layer_id in range(LAYERS - 1, 0, -1):
        d_act = jnp.dot(out_grads[layer_id], weights[layer_id].T, preferred_element_type=jnp.float32).astype(jnp.bfloat16)
        out_grads[layer_id - 1] = gelu_grad(pre_acts[layer_id - 1], d_act)
    a_facs = []
    s_facs = []
    updates = []
    for layer_id in range(LAYERS):
        h_in = layer_inputs[layer_id]
        g_out = out_grads[layer_id]
        a_facs.append(jnp.dot(h_in.T, h_in, preferred_element_type=jnp.float32) / BATCH_TOTAL)
        s_facs.append(jnp.dot(g_out.T, g_out, preferred_element_type=jnp.float32) / BATCH_TOTAL)
        w_grad = jnp.dot(h_in.T, g_out, preferred_element_type=jnp.float32) / BATCH_TOTAL
        a_inv_layer = a_inv[layer_id * D:(layer_id + 1) * D]
        updates.append(jnp.dot(a_inv_layer, jnp.dot(w_grad, s_inv[layer_id])))
    a_new = FACTOR_DECAY * a_old + (1.0 - FACTOR_DECAY) * jnp.concatenate(a_facs, axis=0)
    s_new = FACTOR_DECAY * s_old + (1.0 - FACTOR_DECAY) * jnp.concatenate(s_facs, axis=0)
    return (jnp.stack(updates), a_new, s_new)
```

```python
import jax
import jax.numpy as jnp
from jax import lax
from jax.experimental import pallas as pl
from jax.experimental.pallas import tpu as pltpu
from jax.sharding import PartitionSpec as P

FACTOR_DECAY = 0.75
MESH = pl.DeviceIdType.MESH
F32 = jnp.float32
BF16 = jnp.bfloat16
N_LAYERS = 4
D = 768
STRIP = 192
ROWS = 2048
BLOCK = 512
CHUNK = 256
MBLOCK = 384
PAIR_SLOTS = 2
SLOTS = 7
GELU_C = 0.7978845608028654
GELU_K = 0.044715
CONTRACT_ROWS = (((0,), (0,)), ((), ()))
SCHEDULE = """
F0 F1 F2 B3 B2 P2.3 P2.2 R0 P2.1 R1 B1 R2 S0.1.0 P1.1 S0.1.1 S0.1.2 S1.1.0 P2.0 R3 S1.1.1 S2.1.0 P1.3 R4
S0.2.2 S1.1.2 S1.2.0 S2.1.1 S2.1.2 P1.2 R5 S3.1.0 P0.3 R6 S0.2.0 S0.2.1 S1.2.1 S4.1.0 S3.1.2 P0.0 S1.2.2
S2.2.2 S4.1.1 S3.1.1 S1.3.0 S2.2.0 S5.1.0 S4.1.2 S6.1.0 S6.1.1 S5.1.2 S0.3.2 S3.2.2 S0.3.1 S0.3.0 R7 P0.2
S1.3.1 S4.2.0 S3.2.0 S5.1.1 S6.1.2 S2.2.1 S4.2.2 S4.2.1 S5.2.2 S2.3.2 S1.3.2 R8 P1.0 S3.2.1 S5.2.0 S6.2.0
S6.2.1 S7.1.0 S3.3.2 S2.3.1 S6.2.2 S5.2.1 S4.3.0 S4.3.2 S4.3.1 S7.1.2 S2.3.0 V R9 S3.3.0 S3.3.1 R10 S5.3.0
S6.3.0 S6.3.1 S7.1.1 S8.1.0 P0.1 S5.3.2 S5.3.1 S6.3.2 S7.2.0 S8.1.1 S8.1.2 S7.2.2 S9.1.2 S7.3.2 R11 S9.1.1
S10.1.2 S7.2.1 S7.3.0 S11.1.1 S8.2.1 S10.1.1 S8.2.0 S9.2.1 S11.1.2 U S9.1.0 S10.2.1 S10.1.0 S11.2.1 S8.2.2
S8.3.0 S9.2.2 S11.1.0 f0.2 f0.4 S10.2.2 S8.3.1 f1.4 f2.4 S11.2.2 S9.3.1 f1.2 f2.2 f3.4 S7.3.1 S11.2.0 f0.1
f3.2 f0.6 f2.6 S9.2.0 S8.3.2 S11.3.2 S11.3.0 f1.1 f2.1 S10.2.0 S10.3.2 S10.3.1 f0.5 S11.3.1 f3.1 f2.3 S9.3.2
f3.6 f1.6 S9.3.0 f0.3 f3.5 f1.5 f2.5 f1.3 S10.3.0 f3.3 f2.7 f3.7 f1.7 f0.7
""".split()
PRODUCTS = [(int(e[1]), int(e[3])) for e in SCHEDULE if e[0] == "P"]
N_PROD = len(PRODUCTS)
EARLY = 1
FIRST_LATE = 3
ORDERS = [(1, 2, 4), (2, 4, 1), (4, 1, 2)]
WIDE = 128
PIECES = [(0, 256, (1, 2, 4)), (256, 256, (1, 4, 2)), (512, 256, (2, 1, 4)), (768, 128, (2, 4, 1))]


def xor_chip(chip, mask):
    out = chip
    for bit in (1, 2, 4):
        if mask & bit:
            out = out + bit - 2 * bit * lax.rem(lax.div(chip, bit), 2)
    return out


def unit(j, step, layer, tx):
    bits = {1: tx, 2: layer % 2, 4: layer // 2}
    index = (0, 4, 6)[step]
    for place, dim in enumerate(ORDERS[j][step + 1:]):
        index = index + bits[dim] * (place + 1)
    return index


def cols(j):
    return pl.ds(j * CHUNK, CHUNK)


def kernel(x_hbm, dy_hbm, w_hbm, ainv_hbm, sinv_hbm, u_hbm, a_out, s_out,
           act, wts, part, pair_buf, acc, stg, recv_g, recv_as, gsum, sinv, ainv, vfull, ustrip,
           load_sem, pair_send, pair_recv, credit, send_sem, recv_sem,
           v_send, v_recv, v_fwd_send, v_fwd_recv, v_pair_send, v_pair_recv,
           g_send, g_recv, gp_send, gp_recv, loc_sem):
    me = lax.axis_index("data")
    core = lax.rem(me, 2)
    chip = lax.div(me, 2)
    xbit = lax.rem(chip, 2)
    ybit = lax.rem(lax.div(chip, 2), 2)
    zbit = lax.div(chip, 4)
    layer_own = lax.div(chip, 2)
    partner = chip * 2 + 1 - core

    def peer(mask):
        return xor_chip(chip, mask) * 2 + core

    loads = [
        pltpu.make_async_copy(x_hbm, act.at[0], load_sem.at[0]),
        pltpu.make_async_copy(w_hbm, wts, load_sem.at[1]),
        pltpu.make_async_copy(dy_hbm, act.at[7], load_sem.at[2]),
        pltpu.make_async_copy(ainv_hbm, ainv, load_sem.at[3]),
        pltpu.make_async_copy(sinv_hbm.at[layer_own], sinv, load_sem.at[4]),
    ]
    for ld in loads:
        ld.start()

    barrier = pltpu.get_barrier_semaphore()
    pl.semaphore_signal(barrier, inc=1, device_id=(partner,), device_id_type=MESH)
    for mask in (1, 2, 4):
        pl.semaphore_signal(barrier, inc=1, device_id=(peer(mask),), device_id_type=MESH)
    pl.semaphore_wait(barrier, 4)


    def pair_copy(p, tx):
        row = pl.multiple_of((2 * tx + 1 - core) * STRIP, STRIP)
        return pltpu.make_async_remote_copy(
            src_ref=part.at[p % 2, pl.ds(row, STRIP)],
            dst_ref=pair_buf.at[p % PAIR_SLOTS, tx],
            send_sem=pair_send.at[p % 2, tx],
            recv_sem=pair_recv.at[p % PAIR_SLOTS, tx],
            device_id=(partner,),
            device_id_type=MESH,
        )

    def landing(kind, j, u):
        return recv_g.at[j, u] if kind == 2 else recv_as.at[kind, j, u]

    def staged(p, tx, j):
        if p < FIRST_LATE:
            return stg, (sum(k != 2 for k, _ in PRODUCTS[:p]), tx, slice(None), cols(j))
        n = sum(k != 2 for k, _ in PRODUCTS[FIRST_LATE:p])
        return wts, (n // 2, pl.ds((n % 2) * 2 * STRIP + tx * STRIP, STRIP), cols(j))

    def strip_copy(p, j, step, tx):
        kind, layer = PRODUCTS[p]
        u = unit(j, step, layer, tx)
        if kind == 2:
            src = acc.at[p % SLOTS, tx, :, cols(j)]
        else:
            ref, idx = staged(p, tx, j)
            src = ref.at[idx]
        return pltpu.make_async_remote_copy(
            src_ref=src,
            dst_ref=landing(kind, j, u),
            send_sem=send_sem.at[p % SLOTS, j, tx],
            recv_sem=recv_sem.at[kind, j, u],
            device_id=(peer(ORDERS[j][step]),),
            device_id_type=MESH,
        )

    def product(p):
        kind, layer = PRODUCTS[p]
        left = layer if kind != 1 else 4 + layer
        right = layer if kind == 0 else 4 + layer

        def body(mb, carry):
            ms = pl.ds(pl.multiple_of(mb * MBLOCK, MBLOCK), MBLOCK)
            part[p % 2, ms] = lax.dot_general(act[left, :, ms], act[right], CONTRACT_ROWS,
                                              preferred_element_type=F32)
            return carry
        lax.fori_loop(0, D // MBLOCK, body, 0)
        if p >= PAIR_SLOTS:
            pl.semaphore_wait(credit, 1)
        for tx in range(2):
            pair_copy(p, tx).start()

    def drain(p):
        _, layer = PRODUCTS[p]
        for j in range(3):
            strip_copy(p, j, 0, 1 - xbit).wait_send()

        @pl.when(layer_own != layer)
        def _():
            for j in range(3):
                strip_copy(p, j, 0, xbit).wait_send()

    def equal(dim, layer):
        z_l, y_l = divmod(layer, 2)
        return ybit == y_l if dim == 2 else zbit == z_l

    def stage(p, step, chunks=(0, 1, 2)):
        kind, layer = PRODUCTS[p]
        slot = p % SLOTS
        for j in chunks:
            order = ORDERS[j]
            before = order[:step]
            active = None
            for dim in before:
                if dim != 1:
                    cond = equal(dim, layer)
                    active = cond if active is None else jnp.logical_and(active, cond)
            strips = [xbit] if 1 in before else [0, 1]

            def body(j=j, order=order, strips=strips):
                if step > 0:
                    for tx in strips:
                        strip_copy(p, j, step - 1, tx).wait_recv()
                        u = unit(j, step - 1, layer, tx)
                        got = recv_g[j, u] if kind == 2 else recv_as[kind, j, u].astype(F32)
                        new = acc[slot, tx, :, cols(j)] + got
                        if step < 3:
                            acc[slot, tx, :, cols(j)] = new
                        if kind != 2 and step < 3:
                            ref, idx = staged(p, tx, j)
                            ref[idx] = new.astype(BF16)
                if step == 3:
                    if kind == 2:
                        gsum[:, cols(j)] = new * (1.0 / (ROWS * 16))
                    elif kind == 0:
                        a_out[:, cols(j)] = new
                    else:
                        s_out[:, cols(j)] = new
                    return
                dim = order[step]
                if dim == 1:
                    strip_copy(p, j, step, 1 - xbit).start()
                else:
                    @pl.when(jnp.logical_not(equal(dim, layer)))
                    def _():
                        for tx in strips:
                            strip_copy(p, j, step, tx).start()

            if active is None:
                body()
            else:
                pl.when(active)(body)
    def pair_sum(p):
        kind, layer = PRODUCTS[p]
        slot = p % SLOTS
        if p >= SLOTS:
            drain(p - SLOTS)
        for tx in range(2):
            pair_copy(p, tx).wait_recv()
            row = pl.multiple_of((2 * tx + core) * STRIP, STRIP)
            total = part[p % 2, pl.ds(row, STRIP)] + pair_buf[p % PAIR_SLOTS, tx]
            acc[slot, tx] = total
            if kind != 2:
                for j in range(3):
                    ref, idx = staged(p, tx, j)
                    ref[idx] = total[:, j * CHUNK:(j + 1) * CHUNK].astype(BF16)
        stage(p, 0)
        for tx in range(2):
            pair_copy(p, tx).wait_send()
        if p + PAIR_SLOTS < N_PROD:
            pl.semaphore_signal(credit, inc=1, device_id=(partner,), device_id_type=MESH)


    def forward(layer):
        def body(rb, carry):
            rows = pl.ds(pl.multiple_of(rb * BLOCK, BLOCK), BLOCK)
            z = jnp.dot(act[layer, rows], wts[layer], preferred_element_type=F32).astype(BF16)
            act[4 + layer, rows] = z
            act[layer + 1, rows] = jax.nn.gelu(z.astype(F32), approximate=True).astype(BF16)
            return carry
        lax.fori_loop(0, ROWS // BLOCK, body, 0)

    def backward(layer):
        def body(rb, carry):
            rows = pl.ds(pl.multiple_of(rb * BLOCK, BLOCK), BLOCK)
            d_act = lax.dot_general(act[4 + layer, rows], wts[layer], (((1,), (1,)), ((), ())),
                                    preferred_element_type=F32).astype(BF16).astype(F32)
            z = act[3 + layer, rows].astype(F32)
            z2 = z * z
            t = jnp.tanh(GELU_C * (z + GELU_K * (z2 * z)))
            slope = 0.5 * (1.0 + t) + (0.5 * z) * ((1.0 - t * t) * (GELU_C * (1.0 + 3.0 * GELU_K * z2)))
            act[3 + layer, rows] = (d_act * slope).astype(BF16)
            return carry
        lax.fori_loop(0, ROWS // BLOCK, body, 0)


    my_strip = 2 * xbit + core
    pair_strip = 2 * xbit + 1 - core
    far_strip = 2 * (1 - xbit) + core
    far_pair_strip = 2 * (1 - xbit) + 1 - core
    far = peer(1)

    def vblock(strip, j):
        return vfull.at[pl.ds(pl.multiple_of(strip * STRIP, STRIP), STRIP), cols(j)]

    def vcopy(strip, j, ssem, rsem, dev):
        return pltpu.make_async_remote_copy(
            src_ref=vblock(strip, j), dst_ref=vblock(strip, j), send_sem=ssem.at[j], recv_sem=rsem.at[j],
            device_id=(dev,), device_id_type=MESH)

    def v_stage():
        loads[3].wait()
        loads[4].wait()
        for j in range(3):
            vfull[pl.ds(pl.multiple_of(my_strip * STRIP, STRIP), STRIP), cols(j)] = jnp.dot(
                gsum[...], sinv[:, cols(j)], precision=lax.Precision.HIGHEST, preferred_element_type=F32)
            vcopy(my_strip, j, v_send, v_recv, far).start()
            vcopy(my_strip, j, v_pair_send, v_pair_recv, partner).start()

    def u_block(dev, n):
        first, width, _ = PIECES[n]
        return u_hbm.at[pl.ds(pl.multiple_of(dev * STRIP, STRIP), STRIP), pl.ds(first, width)]

    def u_own(n):
        first, width, _ = PIECES[n]
        return ustrip.at[:, pl.ds(first, width)]

    def u_copy(n, dev, src_own, ssem, rsem, target):
        return pltpu.make_async_remote_copy(
            src_ref=u_own(n) if src_own else u_block(dev, n), dst_ref=u_block(dev, n), send_sem=ssem, recv_sem=rsem,
            device_id=(target,), device_id_type=MESH)

    sent = []

    def launch(n, mask, dims):
        dev = peer(mask) if mask else me
        for d in dims:
            m = mask | d
            cp = u_copy(n, dev, mask == 0, g_send.at[n, m], g_recv.at[n, m], peer(d))
            cp.start()
            sent.append(cp)
        cp = u_copy(n, dev, mask == 0, gp_send.at[n, mask], gp_recv.at[n, mask], partner)
        cp.start()
        sent.append(cp)

    local = [pltpu.make_async_copy(u_own(n), u_block(me, n), loc_sem.at[n]) for n in range(4)]

    def u_stage():
        for j in range(3):
            vcopy(far_strip, j, v_send, v_recv, far).wait_recv()
            vcopy(far_strip, j, v_fwd_send, v_fwd_recv, partner).start()
        for j in range(3):
            vcopy(pair_strip, j, v_pair_send, v_pair_recv, partner).wait_recv()
            vcopy(far_pair_strip, j, v_fwd_send, v_fwd_recv, partner).wait_recv()
            u_rows = jnp.dot(ainv[...], vfull[:, cols(j)], precision=lax.Precision.HIGHEST, preferred_element_type=F32)
            high = u_rows.astype(BF16)
            ustrip[:, cols(j)] = high
            pieces = [j]
            if j == 2:
                ustrip[:, D:] = (u_rows - high.astype(F32))[:, CHUNK - WIDE:].astype(BF16)
                pieces = [2, 3]
            for n in pieces:
                launch(n, 0, PIECES[n][2])
                local[n].start()

    def u_forward(n, mask):
        order = PIECES[n][2]
        last = max(i for i in range(3) if mask & order[i])
        u_copy(n, peer(mask), False, g_send.at[n, mask], g_recv.at[n, mask], peer(order[last])).wait_recv()
        launch(n, mask, order[last + 1:])


    waited = set()

    def loaded(n):
        if n not in waited:
            waited.add(n)
            loads[n].wait()

    loaded(0)
    n_prod = 0
    for event in SCHEDULE:
        what, args = event[0], [int(a) for a in event[1:].split(".") if a]
        if what == "P":
            if args[0] == 1 or (args[0] == 2 and args[1] == 3):
                loaded(2)
            product(n_prod)
            n_prod += 1
        elif what == "R":
            pair_sum(args[0])
        elif what == "S":
            stage(args[0], args[1], (args[2],))
        elif what == "F":
            loaded(1)
            forward(args[0])
        elif what == "B":
            loaded(2)
            backward(args[0])
        elif what == "V":
            v_stage()
        elif what == "U":
            u_stage()
        else:
            u_forward(*args)
    for n in range(4):
        for mask in range(8):
            dev = xor_chip(chip, mask) * 2 + 1 - core
            u_copy(n, dev, False, gp_send.at[n, mask], gp_recv.at[n, mask], partner).wait_recv()
    for cp in sent:
        cp.wait_send()
    for cp in local:
        cp.wait()
    for j in range(3):
        vcopy(my_strip, j, v_send, v_recv, far).wait_send()
        vcopy(my_strip, j, v_pair_send, v_pair_recv, partner).wait_send()
        vcopy(far_strip, j, v_fwd_send, v_fwd_recv, partner).wait_send()
    for p in range(N_PROD - SLOTS, N_PROD):
        drain(p)


def solution(mesh):
    dma = pltpu.SemaphoreType.DMA
    any_spec = pl.BlockSpec(memory_space=pl.ANY)
    vmem_spec = pl.BlockSpec(memory_space=pltpu.VMEM)

    def device_step(x_loc, dy_loc, weights, a_old_rows, s_old_rows, a_inv_rows, s_inv):
        u_parts, a_sum, s_sum = pl.pallas_call(
            kernel,
            out_shape=(
                jax.ShapeDtypeStruct((N_LAYERS * D, D + WIDE), BF16),
                jax.ShapeDtypeStruct((STRIP, D), F32),
                jax.ShapeDtypeStruct((STRIP, D), F32),
            ),
            in_specs=[any_spec] * 5,
            out_specs=(any_spec, vmem_spec, vmem_spec),
            scratch_shapes=[
                pltpu.VMEM((8, ROWS, D), BF16),
                pltpu.VMEM((N_LAYERS, D, D), BF16),
                pltpu.VMEM((2, D, D), F32),
                pltpu.VMEM((PAIR_SLOTS, 2, STRIP, D), F32),
                pltpu.VMEM((SLOTS, 2, STRIP, D), F32),
                pltpu.VMEM((EARLY, 2, STRIP, D), BF16),
                pltpu.VMEM((3, 7, STRIP, CHUNK), F32),
                pltpu.VMEM((2, 3, 7, STRIP, CHUNK), BF16),
                pltpu.VMEM((STRIP, D), F32),
                pltpu.VMEM((D, D), F32),
                pltpu.VMEM((STRIP, D), F32),
                pltpu.VMEM((D, D), F32),
                pltpu.VMEM((STRIP, D + WIDE), BF16),
                dma((5,)), dma((2, 2)), dma((PAIR_SLOTS, 2)), pltpu.SemaphoreType.REGULAR,
                dma((SLOTS, 3, 2)), dma((3, 3, 7)),
                dma((3,)), dma((3,)), dma((3,)), dma((3,)), dma((3,)), dma((3,)),
                dma((4, 8)), dma((4, 8)), dma((4, 8)), dma((4, 8)), dma((4,)),
            ],
            compiler_params=pltpu.CompilerParams(
                collective_id=0, has_side_effects=True, vmem_limit_bytes=67043328),
        )(x_loc, dy_loc, weights, a_inv_rows, s_inv)
        scale = (1.0 - FACTOR_DECAY) / (ROWS * 16)
        a_new = FACTOR_DECAY * a_old_rows + scale * a_sum
        s_new = FACTOR_DECAY * s_old_rows + scale * s_sum
        u_flat = u_parts[:, :D].astype(F32) + jnp.pad(u_parts[:, D:].astype(F32), ((0, 0), (D - WIDE, 0)))
        return u_flat.reshape(N_LAYERS, D, D), a_new, s_new

    row_spec = P("data", None)
    return jax.shard_map(
        device_step,
        mesh=mesh,
        in_specs=(row_spec, row_spec, P(), row_spec, row_spec, row_spec, P()),
        out_specs=(P(), row_spec, row_spec),
        check_vma=False,
    )
```

```python
import jax
import jax.numpy as jnp
from jax import lax
from jax.experimental import pallas as pl
from jax.experimental.pallas import tpu as pltpu
from jax.sharding import PartitionSpec as P

FACTOR_DECAY = 0.75
MESH = pl.DeviceIdType.MESH
F32 = jnp.float32
BF16 = jnp.bfloat16
N_LAYERS = 4
D = 768
STRIP = 192
ROWS = 2048
BLOCK = 512
CHUNK = 256
MBLOCK = 384
PAIR_SLOTS = 2
TAIL_STEPS = 4
SLOTS = 7
GELU_C = 0.7978845608028654
GELU_K = 0.044715
CONTRACT_ROWS = (((0,), (0,)), ((), ()))
SCHEDULE = [
    ("F", 0), ("F", 1), ("F", 2), ("B", 3), ("B", 2), ("P", 0, 0), ("P", 2, 2), ("R", 0), ("P", 2, 3), ("R", 1),
    ("P", 2, 1), ("R", 2), ("S", 0, 1, 0), ("S", 0, 1, 1), ("S", 0, 1, 2), ("B", 1), ("R", 3), ("S", 1, 1, 0),
    ("P", 2, 0), ("S", 1, 1, 1), ("S", 1, 1, 2), ("S", 2, 1, 0), ("S", 0, 2, 1), ("P", 1, 2), ("R", 4),
    ("S", 2, 1, 1), ("S", 0, 2, 0), ("S", 0, 2, 2), ("P", 1, 3), ("R", 5), ("S", 1, 2, 0), ("S", 1, 2, 2),
    ("S", 2, 1, 2), ("S", 3, 1, 0), ("S", 3, 1, 2), ("S", 0, 3, 1), ("P", 0, 2), ("R", 6), ("S", 3, 1, 1),
    ("P", 0, 1), ("S", 4, 1, 0), ("S", 4, 1, 1), ("S", 5, 1, 0), ("S", 2, 2, 0), ("S", 2, 2, 1), ("S", 1, 2, 1),
    ("S", 4, 1, 2), ("S", 0, 3, 2), ("S", 3, 2, 2), ("S", 0, 3, 0), ("R", 7), ("P", 1, 1), ("S", 2, 2, 2),
    ("S", 3, 2, 0), ("S", 5, 1, 1), ("S", 5, 1, 2), ("S", 6, 1, 0), ("S", 1, 3, 2), ("S", 1, 3, 0), ("S", 1, 3, 1),
    ("R", 8), ("P", 1, 0), ("S", 4, 2, 0), ("S", 4, 2, 2), ("S", 6, 1, 1), ("S", 6, 1, 2), ("S", 2, 3, 1),
    ("S", 3, 2, 1), ("S", 4, 2, 1), ("S", 5, 2, 0), ("S", 7, 1, 0), ("S", 2, 3, 2), ("S", 2, 3, 0), ("R", 9),
    ("S", 5, 2, 2), ("P", 0, 3), ("S", 3, 3, 2), ("S", 3, 3, 0), ("S", 8, 1, 0), ("S", 7, 1, 2), ("S", 6, 2, 2),
    ("S", 7, 1, 1), ("S", 6, 2, 0), ("S", 4, 3, 1), ("S", 3, 3, 1), ("R", 10), ("S", 8, 1, 2), ("S", 8, 1, 1),
    ("S", 9, 1, 0), ("S", 4, 3, 0), ("S", 4, 3, 2), ("V",), ("R", 11), ("S", 5, 2, 1), ("S", 6, 2, 1),
    ("S", 7, 2, 0), ("S", 7, 2, 2), ("S", 5, 3, 2), ("S", 5, 3, 0), ("S", 6, 3, 0), ("S", 10, 1, 0), ("S", 9, 1, 2),
    ("S", 8, 2, 2), ("S", 9, 1, 1), ("S", 8, 2, 0), ("S", 6, 3, 2), ("S", 9, 2, 0), ("S", 10, 1, 1), ("S", 7, 2, 1),
    ("S", 7, 3, 2), ("S", 10, 1, 2), ("W", 0), ("U", 0), ("S", 10, 2, 0), ("S", 11, 1, 2), ("S", 8, 2, 1),
    ("S", 11, 1, 1), ("W", 1), ("S", 10, 2, 1), ("S", 7, 3, 0), ("U", 1), ("S", 8, 3, 2), ("S", 9, 2, 1),
    ("f", 0, 2), ("S", 8, 3, 0), ("W", 2), ("S", 10, 3, 0), ("S", 11, 2, 1), ("U", 2), ("S", 9, 3, 0),
    ("S", 11, 1, 0), ("f", 1, 2), ("S", 5, 3, 1), ("f", 0, 4), ("S", 6, 3, 1), ("S", 9, 2, 2), ("f", 1, 4),
    ("S", 7, 3, 1), ("S", 10, 2, 2), ("f", 0, 1), ("f", 2, 2), ("f", 3, 2), ("f", 0, 6), ("S", 8, 3, 1),
    ("f", 2, 4), ("f", 3, 4), ("S", 9, 3, 2), ("S", 11, 2, 0), ("S", 9, 3, 1), ("f", 1, 6), ("S", 10, 3, 1),
    ("S", 11, 3, 1), ("S", 11, 2, 2), ("S", 10, 3, 2), ("f", 1, 1), ("f", 0, 5), ("f", 2, 1), ("f", 2, 6),
    ("f", 0, 3), ("f", 3, 1), ("S", 11, 3, 2), ("f", 3, 6), ("S", 11, 3, 0), ("f", 2, 3), ("f", 1, 3), ("f", 1, 5),
    ("f", 3, 3), ("f", 2, 5), ("f", 0, 7), ("f", 3, 5), ("f", 2, 7), ("f", 1, 7), ("f", 3, 7),
]
PRODUCTS = [event[1:] for event in SCHEDULE if event[0] == "P"]
N_PROD = len(PRODUCTS)
EARLY = 1
FIRST_LATE = 4
ORDERS = [(1, 2, 4), (2, 4, 1), (4, 1, 2)]
WIDE = 128
PIECES = [(0, 256, (1, 2, 4)), (256, 256, (1, 4, 2)), (512, 256, (2, 4, 1)), (768, 128, (1, 2, 4))]


def xor_chip(chip, mask):
    out = chip
    for bit in (1, 2, 4):
        if mask & bit:
            out = out + bit - 2 * bit * lax.rem(lax.div(chip, bit), 2)
    return out


def unit(j, step, layer, tx):
    bits = {1: tx, 2: layer % 2, 4: layer // 2}
    index = (0, 4, 6)[step]
    for place, dim in enumerate(ORDERS[j][step + 1:]):
        index = index + bits[dim] * (place + 1)
    return index


def cols(j):
    return pl.ds(j * CHUNK, CHUNK)


def kernel(x_hbm, dy_hbm, w_hbm, ainv_hbm, sinv_hbm, u_hbm, a_out, s_out,
           act, wts, part, pair_buf, acc, stg, recv_g, recv_as, gsum, sinv, ainv, vfull, ustrip,
           load_sem, pair_send, pair_recv, credit, send_sem, recv_sem,
           v_send, v_recv, v_fwd_send, v_fwd_recv, v_pair_send, v_pair_recv,
           g_send, g_recv, gp_send, gp_recv, loc_sem):
    me = lax.axis_index("data")
    core = lax.rem(me, 2)
    chip = lax.div(me, 2)
    xbit = lax.rem(chip, 2)
    ybit = lax.rem(lax.div(chip, 2), 2)
    zbit = lax.div(chip, 4)
    layer_own = lax.div(chip, 2)
    partner = chip * 2 + 1 - core

    def peer(mask):
        return xor_chip(chip, mask) * 2 + core

    loads = [
        pltpu.make_async_copy(x_hbm, act.at[0], load_sem.at[0]),
        pltpu.make_async_copy(w_hbm, wts, load_sem.at[1]),
        pltpu.make_async_copy(dy_hbm, act.at[7], load_sem.at[2]),
        pltpu.make_async_copy(ainv_hbm, ainv, load_sem.at[3]),
        pltpu.make_async_copy(sinv_hbm.at[layer_own], sinv, load_sem.at[4]),
    ]
    for ld in loads:
        ld.start()

    barrier = pltpu.get_barrier_semaphore()
    pl.semaphore_signal(barrier, inc=1, device_id=(partner,), device_id_type=MESH)
    for mask in (1, 2, 4):
        pl.semaphore_signal(barrier, inc=1, device_id=(peer(mask),), device_id_type=MESH)
    pl.semaphore_wait(barrier, 4)


    def pair_copy(p, tx):
        row = pl.multiple_of((2 * tx + 1 - core) * STRIP, STRIP)
        return pltpu.make_async_remote_copy(
            src_ref=part.at[p % 2, pl.ds(row, STRIP)],
            dst_ref=pair_buf.at[p % PAIR_SLOTS, tx],
            send_sem=pair_send.at[p % 2, tx],
            recv_sem=pair_recv.at[p % PAIR_SLOTS, tx],
            device_id=(partner,),
            device_id_type=MESH,
        )

    def landing(kind, j, u):
        return recv_g.at[j, u] if kind == 2 else recv_as.at[kind, j, u]

    def staged(p, tx, j):
        if p < FIRST_LATE:
            return stg, (sum(k != 2 for k, _ in PRODUCTS[:p]), tx, slice(None), cols(j))
        n = sum(k != 2 for k, _ in PRODUCTS[FIRST_LATE:p])
        return wts, (n // 2, pl.ds((n % 2) * 2 * STRIP + tx * STRIP, STRIP), cols(j))

    def strip_copy(p, j, step, tx):
        kind, layer = PRODUCTS[p]
        u = unit(j, step, layer, tx)
        if kind == 2:
            src = acc.at[p % SLOTS, tx, :, cols(j)]
        else:
            ref, idx = staged(p, tx, j)
            src = ref.at[idx]
        return pltpu.make_async_remote_copy(
            src_ref=src,
            dst_ref=landing(kind, j, u),
            send_sem=send_sem.at[p % SLOTS, j, tx],
            recv_sem=recv_sem.at[kind, j, u],
            device_id=(peer(ORDERS[j][step]),),
            device_id_type=MESH,
        )

    def product(p):
        kind, layer = PRODUCTS[p]
        left = layer if kind != 1 else 4 + layer
        right = layer if kind == 0 else 4 + layer

        def body(mb, carry):
            ms = pl.ds(pl.multiple_of(mb * MBLOCK, MBLOCK), MBLOCK)
            part[p % 2, ms] = lax.dot_general(act[left, :, ms], act[right], CONTRACT_ROWS,
                                              preferred_element_type=F32)
            return carry
        lax.fori_loop(0, D // MBLOCK, body, 0)
        if p >= PAIR_SLOTS:
            pl.semaphore_wait(credit, 1)
        for tx in range(2):
            pair_copy(p, tx).start()

    def drain(p):
        _, layer = PRODUCTS[p]
        for j in range(3):
            strip_copy(p, j, 0, 1 - xbit).wait_send()

        @pl.when(layer_own != layer)
        def _():
            for j in range(3):
                strip_copy(p, j, 0, xbit).wait_send()

    def equal(dim, layer):
        z_l, y_l = divmod(layer, 2)
        return ybit == y_l if dim == 2 else zbit == z_l

    def stage(p, step, chunks=(0, 1, 2)):
        kind, layer = PRODUCTS[p]
        slot = p % SLOTS
        for j in chunks:
            order = ORDERS[j]
            before = order[:step]
            active = None
            for dim in before:
                if dim != 1:
                    cond = equal(dim, layer)
                    active = cond if active is None else jnp.logical_and(active, cond)
            strips = [xbit] if 1 in before else [0, 1]

            def body(j=j, order=order, strips=strips):
                if step > 0:
                    for tx in strips:
                        strip_copy(p, j, step - 1, tx).wait_recv()
                        u = unit(j, step - 1, layer, tx)
                        got = recv_g[j, u] if kind == 2 else recv_as[kind, j, u].astype(F32)
                        new = acc[slot, tx, :, cols(j)] + got
                        if step < 3:
                            acc[slot, tx, :, cols(j)] = new
                        if kind != 2 and step < 3:
                            ref, idx = staged(p, tx, j)
                            ref[idx] = new.astype(BF16)
                if step == 3:
                    if kind == 2:
                        gsum[:, cols(j)] = new * (1.0 / (ROWS * 16))
                    elif kind == 0:
                        a_out[:, cols(j)] = new
                    else:
                        s_out[:, cols(j)] = new
                    return
                dim = order[step]
                if dim == 1:
                    strip_copy(p, j, step, 1 - xbit).start()
                else:
                    @pl.when(jnp.logical_not(equal(dim, layer)))
                    def _():
                        for tx in strips:
                            strip_copy(p, j, step, tx).start()

            if active is None:
                body()
            else:
                pl.when(active)(body)
    def pair_sum(p):
        kind, layer = PRODUCTS[p]
        slot = p % SLOTS
        if p >= SLOTS:
            drain(p - SLOTS)
        for tx in range(2):
            pair_copy(p, tx).wait_recv()
            row = pl.multiple_of((2 * tx + core) * STRIP, STRIP)
            total = part[p % 2, pl.ds(row, STRIP)] + pair_buf[p % PAIR_SLOTS, tx]
            acc[slot, tx] = total
            if kind != 2:
                for j in range(3):
                    ref, idx = staged(p, tx, j)
                    ref[idx] = total[:, j * CHUNK:(j + 1) * CHUNK].astype(BF16)
        stage(p, 0)
        for tx in range(2):
            pair_copy(p, tx).wait_send()
        if p + PAIR_SLOTS < N_PROD:
            pl.semaphore_signal(credit, inc=1, device_id=(partner,), device_id_type=MESH)


    def forward(layer):
        def body(rb, carry):
            rows = pl.ds(pl.multiple_of(rb * BLOCK, BLOCK), BLOCK)
            z = jnp.dot(act[layer, rows], wts[layer], preferred_element_type=F32).astype(BF16)
            act[4 + layer, rows] = z
            zf = z.astype(F32)
            half = 0.5 * zf
            t = jnp.tanh(zf * (GELU_C + (GELU_C * GELU_K) * (zf * zf)))
            act[layer + 1, rows] = (half + half * t).astype(BF16)
            return carry
        lax.fori_loop(0, ROWS // BLOCK, body, 0)

    def backward(layer):
        def body(rb, carry):
            rows = pl.ds(pl.multiple_of(rb * BLOCK, BLOCK), BLOCK)
            d_act = lax.dot_general(act[4 + layer, rows], wts[layer], (((1,), (1,)), ((), ())),
                                    preferred_element_type=F32).astype(BF16).astype(F32)
            z = act[3 + layer, rows].astype(F32)
            z2 = z * z
            t = jnp.tanh(z * (GELU_C + (GELU_C * GELU_K) * z2))
            slope = (0.5 + 0.5 * t) + (0.5 * z) * ((1.0 - t * t) * (GELU_C + (3.0 * GELU_C * GELU_K) * z2))
            act[3 + layer, rows] = (d_act * slope).astype(BF16)
            return carry
        lax.fori_loop(0, ROWS // BLOCK, body, 0)


    my_strip = 2 * xbit + core
    pair_strip = 2 * xbit + 1 - core
    far_strip = 2 * (1 - xbit) + core
    far_pair_strip = 2 * (1 - xbit) + 1 - core
    far = peer(1)

    def vblock(strip, j):
        return vfull.at[pl.ds(pl.multiple_of(strip * STRIP, STRIP), STRIP), cols(j)]

    def vcopy(strip, j, ssem, rsem, dev):
        return pltpu.make_async_remote_copy(
            src_ref=vblock(strip, j), dst_ref=vblock(strip, j), send_sem=ssem.at[j], recv_sem=rsem.at[j],
            device_id=(dev,), device_id_type=MESH)

    def v_stage():
        loads[3].wait()
        loads[4].wait()
        for j in range(3):
            vfull[pl.ds(pl.multiple_of(my_strip * STRIP, STRIP), STRIP), cols(j)] = jnp.dot(
                gsum[...], sinv[:, cols(j)], precision=lax.Precision.HIGHEST, preferred_element_type=F32)
            vcopy(my_strip, j, v_send, v_recv, far).start()
            vcopy(my_strip, j, v_pair_send, v_pair_recv, partner).start()

    def u_block(dev, n):
        first, width, _ = PIECES[n]
        return u_hbm.at[pl.ds(pl.multiple_of(dev * STRIP, STRIP), STRIP), pl.ds(first, width)]

    def u_own(n):
        first, width, _ = PIECES[n]
        return ustrip.at[:, pl.ds(first, width)]

    def u_copy(n, dev, src_own, ssem, rsem, target):
        return pltpu.make_async_remote_copy(
            src_ref=u_own(n) if src_own else u_block(dev, n), dst_ref=u_block(dev, n), send_sem=ssem, recv_sem=rsem,
            device_id=(target,), device_id_type=MESH)

    sent = []

    def launch(n, mask, dims):
        dev = peer(mask) if mask else me
        for d in dims:
            m = mask | d
            cp = u_copy(n, dev, mask == 0, g_send.at[n, m], g_recv.at[n, m], peer(d))
            cp.start()
            sent.append(cp)
        cp = u_copy(n, dev, mask == 0, gp_send.at[n, mask], gp_recv.at[n, mask], partner)
        cp.start()
        sent.append(cp)

    local = [pltpu.make_async_copy(u_own(n), u_block(me, n), loc_sem.at[n]) for n in range(4)]

    def v_pass(j):
        vcopy(far_strip, j, v_send, v_recv, far).wait_recv()
        vcopy(far_strip, j, v_fwd_send, v_fwd_recv, partner).start()

    def u_stage(j):
        vcopy(pair_strip, j, v_pair_send, v_pair_recv, partner).wait_recv()
        vcopy(far_pair_strip, j, v_fwd_send, v_fwd_recv, partner).wait_recv()
        u_rows = jnp.dot(ainv[...], vfull[:, cols(j)], precision=lax.Precision.HIGHEST, preferred_element_type=F32)
        high = u_rows.astype(BF16)
        ustrip[:, cols(j)] = high
        pieces = [j]
        if j == 2:
            ustrip[:, D:] = (u_rows - high.astype(F32))[:, CHUNK - WIDE:].astype(BF16)
            pieces = [2, 3]
        for n in pieces:
            launch(n, 0, PIECES[n][2])
            local[n].start()

    def u_forward(n, mask):
        order = PIECES[n][2]
        last = max(i for i in range(3) if mask & order[i])
        u_copy(n, peer(mask), False, g_send.at[n, mask], g_recv.at[n, mask], peer(order[last])).wait_recv()
        launch(n, mask, order[last + 1:])


    waited = set()

    def loaded(n):
        if n not in waited:
            waited.add(n)
            loads[n].wait()

    loaded(0)
    n_prod = 0
    for event in SCHEDULE:
        what, args = event[0], event[1:]
        if what == "P":
            if args[0] == 1 or (args[0] == 2 and args[1] == 3):
                loaded(2)
            product(n_prod)
            n_prod += 1
        elif what == "R":
            pair_sum(args[0])
        elif what == "S":
            stage(args[0], args[1], (args[2],))
        elif what == "F":
            loaded(1)
            forward(args[0])
        elif what == "B":
            loaded(2)
            backward(args[0])
        elif what == "V":
            v_stage()
        elif what == "U":
            u_stage(args[0])
        elif what == "W":
            v_pass(args[0])
        else:
            u_forward(*args)
    for n in range(4):
        for mask in range(8):
            dev = xor_chip(chip, mask) * 2 + 1 - core
            u_copy(n, dev, False, gp_send.at[n, mask], gp_recv.at[n, mask], partner).wait_recv()
    for cp in sent:
        cp.wait_send()
    for cp in local:
        cp.wait()
    for j in range(3):
        vcopy(my_strip, j, v_send, v_recv, far).wait_send()
        vcopy(my_strip, j, v_pair_send, v_pair_recv, partner).wait_send()
        vcopy(far_strip, j, v_fwd_send, v_fwd_recv, partner).wait_send()
    for p in range(N_PROD - SLOTS, N_PROD):
        drain(p)


def tail(u_ref, a_old, a_sum, s_old, s_sum, u_out, a_new, s_new):
    scale = (1.0 - FACTOR_DECAY) / (ROWS * 16)
    u_out[:, :D - WIDE] = u_ref[:, :D - WIDE].astype(F32)
    u_out[:, D - WIDE:] = u_ref[:, D - WIDE:D].astype(F32) + u_ref[:, D:].astype(F32)
    a_new[...] = FACTOR_DECAY * a_old[...] + scale * a_sum[...]
    s_new[...] = FACTOR_DECAY * s_old[...] + scale * s_sum[...]


def solution(mesh):
    dma = pltpu.SemaphoreType.DMA
    any_spec = pl.BlockSpec(memory_space=pl.ANY)
    vmem_spec = pl.BlockSpec(memory_space=pltpu.VMEM)

    def device_step(x_loc, dy_loc, weights, a_old_rows, s_old_rows, a_inv_rows, s_inv):
        u_parts, a_sum, s_sum = pl.pallas_call(
            kernel,
            out_shape=(
                jax.ShapeDtypeStruct((N_LAYERS * D, D + WIDE), BF16),
                jax.ShapeDtypeStruct((STRIP, D), F32),
                jax.ShapeDtypeStruct((STRIP, D), F32),
            ),
            in_specs=[any_spec] * 5,
            out_specs=(any_spec, vmem_spec, vmem_spec),
            scratch_shapes=[
                pltpu.VMEM((8, ROWS, D), BF16),
                pltpu.VMEM((N_LAYERS, D, D), BF16),
                pltpu.VMEM((2, D, D), F32),
                pltpu.VMEM((PAIR_SLOTS, 2, STRIP, D), F32),
                pltpu.VMEM((SLOTS, 2, STRIP, D), F32),
                pltpu.VMEM((EARLY, 2, STRIP, D), BF16),
                pltpu.VMEM((3, 7, STRIP, CHUNK), F32),
                pltpu.VMEM((2, 3, 7, STRIP, CHUNK), BF16),
                pltpu.VMEM((STRIP, D), F32),
                pltpu.VMEM((D, D), F32),
                pltpu.VMEM((STRIP, D), F32),
                pltpu.VMEM((D, D), F32),
                pltpu.VMEM((STRIP, D + WIDE), BF16),
                dma((5,)), dma((2, 2)), dma((PAIR_SLOTS, 2)), pltpu.SemaphoreType.REGULAR,
                dma((SLOTS, 3, 2)), dma((3, 3, 7)),
                dma((3,)), dma((3,)), dma((3,)), dma((3,)), dma((3,)), dma((3,)),
                dma((4, 8)), dma((4, 8)), dma((4, 8)), dma((4, 8)), dma((4,)),
            ],
            compiler_params=pltpu.CompilerParams(
                collective_id=0, has_side_effects=True, vmem_limit_bytes=67043328),
        )(x_loc, dy_loc, weights, a_inv_rows, s_inv)
        u_block = pl.BlockSpec((N_LAYERS * D // TAIL_STEPS, D + WIDE), lambda i: (i, 0))
        out_block = pl.BlockSpec((N_LAYERS * D // TAIL_STEPS, D), lambda i: (i, 0))
        row_block = pl.BlockSpec((STRIP // TAIL_STEPS, D), lambda i: (i, 0))
        u_flat, a_new, s_new = pl.pallas_call(
            tail,
            grid=(TAIL_STEPS,),
            out_shape=(
                jax.ShapeDtypeStruct((N_LAYERS * D, D), F32),
                jax.ShapeDtypeStruct((STRIP, D), F32),
                jax.ShapeDtypeStruct((STRIP, D), F32),
            ),
            in_specs=[u_block] + [row_block] * 4,
            out_specs=(out_block, row_block, row_block),
        )(u_parts, a_old_rows, a_sum, s_old_rows, s_sum)
        return u_flat.reshape(N_LAYERS, D, D), a_new, s_new

    row_spec = P("data", None)
    return jax.shard_map(
        device_step,
        mesh=mesh,
        in_specs=(row_spec, row_spec, P(), row_spec, row_spec, row_spec, P()),
        out_specs=(P(), row_spec, row_spec),
        check_vma=False,
    )
```

```python
import jax
import jax.numpy as jnp
from jax import lax
from jax.experimental import pallas as pl
from jax.experimental.pallas import tpu as pltpu
from jax.sharding import PartitionSpec as P

FACTOR_DECAY = 0.75
MESH = pl.DeviceIdType.MESH
F32 = jnp.float32
BF16 = jnp.bfloat16
N_LAYERS = 4
D = 768
STRIP = 192
ROWS = 2048
BLOCK = 512
CHUNK = 256
MBLOCK = 384
PAIR_SLOTS = 2
TAIL_STEPS = 4
SLOTS = 7
GELU_C = 0.7978845608028654
GELU_K = 0.044715
CONTRACT_ROWS = (((0,), (0,)), ((), ()))
SCHEDULE = [
    "F0 F1 F2 B3", "B2 P0.0 P2.2 R0", "P2.3 R1 P2.1 R2", "S0.1.0 S0.1.1 S0.1.2 B1", "R3 S1.1.0 P2.0 S1.1.1",
    "S1.1.2 S2.1.0 S0.2.1 P1.2", "R4 S2.1.1 S0.2.0 S0.2.2", "P1.3 R5 S1.2.0 S1.2.2", "S2.1.2 S3.1.0 S3.1.2 S0.3.1",
    "P0.2 R6 S3.1.1 P0.1", "S4.1.0 S4.1.1 S5.1.0 S2.2.0", "S2.2.1 S1.2.1 S4.1.2 S0.3.2", "S3.2.2 S0.3.0 R7 P1.1",
    "S2.2.2 S3.2.0 S5.1.1 S5.1.2", "S6.1.0 S1.3.2 S1.3.0 S1.3.1", "R8 P1.0 S4.2.0 S4.2.2",
    "S6.1.1 S6.1.2 S2.3.1 S3.2.1", "S4.2.1 S5.2.0 S7.1.0 S2.3.2", "S2.3.0 R9 S5.2.2 P0.3",
    "S3.3.2 S3.3.0 S8.1.0 S7.1.2", "S6.2.2 S7.1.1 S6.2.0 S4.3.1", "S3.3.1 R10 S8.1.2 S8.1.1",
    "S9.1.0 S4.3.0 S4.3.2 V", "R11 S5.2.1 S6.2.1 S7.2.0", "S7.2.2 S5.3.2 S5.3.0 S6.3.0",
    "S10.1.0 S9.1.2 S8.2.2 S9.1.1", "S8.2.0 S6.3.2 S9.2.0 S10.1.1", "S7.2.1 S7.3.2 S10.1.2 W0",
    "U0 S10.2.0 S11.1.2 S8.2.1", "S11.1.1 W1 S10.2.1 S7.3.0", "U1 S8.3.2 S9.2.1 f0.2", "S8.3.0 W2 S10.3.0 S11.2.1",
    "U2 S9.3.0 S11.1.0 f1.2", "S5.3.1 f0.4 S6.3.1 S9.2.2", "f1.4 S7.3.1 S10.2.2 f0.1", "f2.2 f3.2 f0.6 S8.3.1",
    "f2.4 f3.4 S9.3.2 S11.2.0", "S9.3.1 f1.6 S10.3.1 S11.3.1", "S11.2.2 S10.3.2 f1.1 f0.5", "f2.1 f2.6 f0.3 f3.1",
    "S11.3.2 f3.6 S11.3.0 f2.3", "f1.3 f1.5 f3.3 f2.5", "f0.7 f3.5 f2.7 f1.7", "f3.7",
]
EVENTS = [(e[0], [int(a) for a in e[1:].split(".") if a]) for group in SCHEDULE for e in group.split()]
PRODUCTS = [tuple(args) for what, args in EVENTS if what == "P"]
N_PROD = len(PRODUCTS)
EARLY = 1
FIRST_LATE = 4
ORDERS = [(1, 2, 4), (2, 4, 1), (4, 1, 2)]
WIDE = 128
PIECES = [(0, 256, (1, 2, 4)), (256, 256, (1, 4, 2)), (512, 256, (2, 4, 1)), (768, 128, (1, 2, 4))]


def xor_chip(chip, mask):
    out = chip
    for bit in (1, 2, 4):
        if mask & bit:
            out = out + bit - 2 * bit * lax.rem(lax.div(chip, bit), 2)
    return out


def unit(j, step, layer, tx):
    bits = {1: tx, 2: layer % 2, 4: layer // 2}
    index = (0, 4, 6)[step]
    for place, dim in enumerate(ORDERS[j][step + 1:]):
        index = index + bits[dim] * (place + 1)
    return index


def cols(j):
    return pl.ds(j * CHUNK, CHUNK)


def kernel(x_hbm, dy_hbm, w_hbm, ainv_hbm, sinv_hbm, u_hbm, a_out, s_out,
           act, wts, part, pair_buf, acc, stg, recv_g, recv_as, recv_late, gsum, sinv, ainv, vfull, ustrip,
           load_sem, pair_send, pair_recv, credit, send_sem, recv_sem,
           v_send, v_recv, v_fwd_send, v_fwd_recv, v_pair_send, v_pair_recv,
           g_send, g_recv, gp_send, gp_recv, loc_sem):
    me = lax.axis_index("data")
    core = lax.rem(me, 2)
    chip = lax.div(me, 2)
    xbit = lax.rem(chip, 2)
    ybit = lax.rem(lax.div(chip, 2), 2)
    zbit = lax.div(chip, 4)
    layer_own = lax.div(chip, 2)
    partner = chip * 2 + 1 - core

    def peer(mask):
        return xor_chip(chip, mask) * 2 + core

    loads = [
        pltpu.make_async_copy(x_hbm, act.at[0], load_sem.at[0]),
        pltpu.make_async_copy(w_hbm, wts, load_sem.at[1]),
        pltpu.make_async_copy(dy_hbm, act.at[7], load_sem.at[2]),
        pltpu.make_async_copy(ainv_hbm, ainv, load_sem.at[3]),
        pltpu.make_async_copy(sinv_hbm.at[layer_own], sinv, load_sem.at[4]),
    ]
    for ld in loads:
        ld.start()

    barrier = pltpu.get_barrier_semaphore()
    pl.semaphore_signal(barrier, inc=1, device_id=(partner,), device_id_type=MESH)
    for mask in (1, 2, 4):
        pl.semaphore_signal(barrier, inc=1, device_id=(peer(mask),), device_id_type=MESH)
    pl.semaphore_wait(barrier, 4)


    def pair_copy(p, tx):
        row = pl.multiple_of((2 * tx + 1 - core) * STRIP, STRIP)
        return pltpu.make_async_remote_copy(
            src_ref=part.at[p % 2, pl.ds(row, STRIP)],
            dst_ref=pair_buf.at[p % PAIR_SLOTS, tx],
            send_sem=pair_send.at[p % 2, tx],
            recv_sem=pair_recv.at[p % PAIR_SLOTS, tx],
            device_id=(partner,),
            device_id_type=MESH,
        )

    def landing(kind, j, u, step):
        if kind != 2 and step > 0:
            return recv_late.at[kind, j, u - 4]
        return recv_g.at[j, u] if kind == 2 else recv_as.at[kind, j, u]

    def staged(p, tx, j):
        if p < FIRST_LATE:
            return stg, (sum(k != 2 for k, _ in PRODUCTS[:p]), tx, slice(None), cols(j))
        n = sum(k != 2 for k, _ in PRODUCTS[FIRST_LATE:p])
        return wts, (n // 2, pl.ds((n % 2) * 2 * STRIP + tx * STRIP, STRIP), cols(j))

    def strip_copy(p, j, step, tx):
        kind, layer = PRODUCTS[p]
        u = unit(j, step, layer, tx)
        if kind == 2 or step > 0:
            src = acc.at[p % SLOTS, tx, :, cols(j)]
        else:
            ref, idx = staged(p, tx, j)
            src = ref.at[idx]
        return pltpu.make_async_remote_copy(
            src_ref=src,
            dst_ref=landing(kind, j, u, step),
            send_sem=send_sem.at[p % SLOTS, j, tx],
            recv_sem=recv_sem.at[kind, j, u],
            device_id=(peer(ORDERS[j][step]),),
            device_id_type=MESH,
        )

    def product(p):
        kind, layer = PRODUCTS[p]
        left = layer if kind != 1 else 4 + layer
        right = layer if kind == 0 else 4 + layer

        def body(mb, carry):
            ms = pl.ds(pl.multiple_of(mb * MBLOCK, MBLOCK), MBLOCK)
            part[p % 2, ms] = lax.dot_general(act[left, :, ms], act[right], CONTRACT_ROWS,
                                              preferred_element_type=F32)
            return carry
        lax.fori_loop(0, D // MBLOCK, body, 0)
        if p >= PAIR_SLOTS:
            pl.semaphore_wait(credit, 1)
        for tx in range(2):
            pair_copy(p, tx).start()

    def equal(dim, layer):
        z_l, y_l = divmod(layer, 2)
        return ybit == y_l if dim == 2 else zbit == z_l

    def drain(p):
        _, layer = PRODUCTS[p]
        for j in range(3):
            for step, dim in enumerate(ORDERS[j]):
                before = ORDERS[j][:step]
                sent_here = chip >= 0
                for other in before:
                    if other != 1:
                        sent_here = jnp.logical_and(sent_here, equal(other, layer))
                strips = [xbit] if 1 in before else [0, 1]
                if dim == 1:
                    strips = [1 - xbit]
                else:
                    sent_here = jnp.logical_and(sent_here, jnp.logical_not(equal(dim, layer)))

                @pl.when(sent_here)
                def _(j=j, step=step, strips=strips):
                    for tx in strips:
                        strip_copy(p, j, step, tx).wait_send()

    def stage(p, step, chunks=(0, 1, 2)):
        kind, layer = PRODUCTS[p]
        slot = p % SLOTS
        for j in chunks:
            order = ORDERS[j]
            before = order[:step]
            active = None
            for dim in before:
                if dim != 1:
                    cond = equal(dim, layer)
                    active = cond if active is None else jnp.logical_and(active, cond)
            strips = [xbit] if 1 in before else [0, 1]

            def body(j=j, order=order, strips=strips):
                if step > 0:
                    for tx in strips:
                        strip_copy(p, j, step - 1, tx).wait_recv()
                        u = unit(j, step - 1, layer, tx)
                        got = landing(kind, j, u, step - 1)[...].astype(F32)
                        new = acc[slot, tx, :, cols(j)] + got
                        if step < 3:
                            acc[slot, tx, :, cols(j)] = new
                if step == 3:
                    if kind == 2:
                        gsum[:, cols(j)] = new * (1.0 / (ROWS * 16))
                    elif kind == 0:
                        a_out[:, cols(j)] = new
                    else:
                        s_out[:, cols(j)] = new
                    return
                dim = order[step]
                if dim == 1:
                    strip_copy(p, j, step, 1 - xbit).start()
                else:
                    @pl.when(jnp.logical_not(equal(dim, layer)))
                    def _():
                        for tx in strips:
                            strip_copy(p, j, step, tx).start()

            if active is None:
                body()
            else:
                pl.when(active)(body)
    def pair_sum(p):
        kind, layer = PRODUCTS[p]
        slot = p % SLOTS
        if p >= SLOTS:
            drain(p - SLOTS)
        for tx in range(2):
            pair_copy(p, tx).wait_recv()
            row = pl.multiple_of((2 * tx + core) * STRIP, STRIP)
            total = part[p % 2, pl.ds(row, STRIP)] + pair_buf[p % PAIR_SLOTS, tx]
            acc[slot, tx] = total
            if kind != 2:
                for j in range(3):
                    ref, idx = staged(p, tx, j)
                    ref[idx] = total[:, j * CHUNK:(j + 1) * CHUNK].astype(BF16)
        stage(p, 0)
        for tx in range(2):
            pair_copy(p, tx).wait_send()
        if p + PAIR_SLOTS < N_PROD:
            pl.semaphore_signal(credit, inc=1, device_id=(partner,), device_id_type=MESH)


    def forward(layer):
        def body(rb, carry):
            rows = pl.ds(pl.multiple_of(rb * BLOCK, BLOCK), BLOCK)
            z = jnp.dot(act[layer, rows], wts[layer], preferred_element_type=F32).astype(BF16)
            act[4 + layer, rows] = z
            zf = z.astype(F32)
            half = 0.5 * zf
            t = jnp.tanh(zf * (GELU_C + (GELU_C * GELU_K) * (zf * zf)))
            act[layer + 1, rows] = (half + half * t).astype(BF16)
            return carry
        lax.fori_loop(0, ROWS // BLOCK, body, 0)

    def backward(layer):
        def body(rb, carry):
            rows = pl.ds(pl.multiple_of(rb * BLOCK, BLOCK), BLOCK)
            d_act = lax.dot_general(act[4 + layer, rows], wts[layer], (((1,), (1,)), ((), ())),
                                    preferred_element_type=F32).astype(BF16).astype(F32)
            z = act[3 + layer, rows].astype(F32)
            z2 = z * z
            t = jnp.tanh(z * (GELU_C + (GELU_C * GELU_K) * z2))
            slope = (0.5 + 0.5 * t) + (0.5 * z) * ((1.0 - t * t) * (GELU_C + (3.0 * GELU_C * GELU_K) * z2))
            act[3 + layer, rows] = (d_act * slope).astype(BF16)
            return carry
        lax.fori_loop(0, ROWS // BLOCK, body, 0)


    my_strip = 2 * xbit + core
    pair_strip = 2 * xbit + 1 - core
    far_strip = 2 * (1 - xbit) + core
    far_pair_strip = 2 * (1 - xbit) + 1 - core
    far = peer(1)

    def vblock(strip, j):
        return vfull.at[pl.ds(pl.multiple_of(strip * STRIP, STRIP), STRIP), cols(j)]

    def vcopy(strip, j, ssem, rsem, dev):
        return pltpu.make_async_remote_copy(
            src_ref=vblock(strip, j), dst_ref=vblock(strip, j), send_sem=ssem.at[j], recv_sem=rsem.at[j],
            device_id=(dev,), device_id_type=MESH)

    def v_stage():
        loads[3].wait()
        loads[4].wait()
        for j in range(3):
            vfull[pl.ds(pl.multiple_of(my_strip * STRIP, STRIP), STRIP), cols(j)] = jnp.dot(
                gsum[...], sinv[:, cols(j)], precision=lax.Precision.HIGHEST, preferred_element_type=F32)
            vcopy(my_strip, j, v_send, v_recv, far).start()
            vcopy(my_strip, j, v_pair_send, v_pair_recv, partner).start()

    def u_block(dev, n):
        first, width, _ = PIECES[n]
        return u_hbm.at[pl.ds(pl.multiple_of(dev * STRIP, STRIP), STRIP), pl.ds(first, width)]

    def u_own(n):
        first, width, _ = PIECES[n]
        return ustrip.at[:, pl.ds(first, width)]

    def u_copy(n, dev, src_own, ssem, rsem, target):
        return pltpu.make_async_remote_copy(
            src_ref=u_own(n) if src_own else u_block(dev, n), dst_ref=u_block(dev, n), send_sem=ssem, recv_sem=rsem,
            device_id=(target,), device_id_type=MESH)

    sent = []

    def launch(n, mask, dims):
        dev = peer(mask) if mask else me
        for d in dims:
            m = mask | d
            cp = u_copy(n, dev, mask == 0, g_send.at[n, m], g_recv.at[n, m], peer(d))
            cp.start()
            sent.append(cp)
        cp = u_copy(n, dev, mask == 0, gp_send.at[n, mask], gp_recv.at[n, mask], partner)
        cp.start()
        sent.append(cp)

    local = [pltpu.make_async_copy(u_own(n), u_block(me, n), loc_sem.at[n]) for n in range(4)]

    def v_pass(j):
        vcopy(far_strip, j, v_send, v_recv, far).wait_recv()
        vcopy(far_strip, j, v_fwd_send, v_fwd_recv, partner).start()

    def u_stage(j):
        vcopy(pair_strip, j, v_pair_send, v_pair_recv, partner).wait_recv()
        vcopy(far_pair_strip, j, v_fwd_send, v_fwd_recv, partner).wait_recv()
        u_rows = jnp.dot(ainv[...], vfull[:, cols(j)], precision=lax.Precision.HIGHEST, preferred_element_type=F32)
        high = u_rows.astype(BF16)
        ustrip[:, cols(j)] = high
        pieces = [j]
        if j == 2:
            ustrip[:, D:] = (u_rows - high.astype(F32))[:, CHUNK - WIDE:].astype(BF16)
            pieces = [2, 3]
        for n in pieces:
            launch(n, 0, PIECES[n][2])
            local[n].start()

    def u_forward(n, mask):
        order = PIECES[n][2]
        last = max(i for i in range(3) if mask & order[i])
        u_copy(n, peer(mask), False, g_send.at[n, mask], g_recv.at[n, mask], peer(order[last])).wait_recv()
        launch(n, mask, order[last + 1:])


    waited = set()

    def loaded(n):
        if n not in waited:
            waited.add(n)
            loads[n].wait()

    loaded(0)
    n_prod = 0
    for what, args in EVENTS:
        if what == "P":
            if args[0] == 1 or (args[0] == 2 and args[1] == 3):
                loaded(2)
            product(n_prod)
            n_prod += 1
        elif what == "R":
            pair_sum(args[0])
        elif what == "S":
            stage(args[0], args[1], (args[2],))
        elif what == "F":
            loaded(1)
            forward(args[0])
        elif what == "B":
            loaded(2)
            backward(args[0])
        elif what == "V":
            v_stage()
        elif what == "U":
            u_stage(args[0])
        elif what == "W":
            v_pass(args[0])
        else:
            u_forward(*args)
    for n in range(4):
        for mask in range(8):
            dev = xor_chip(chip, mask) * 2 + 1 - core
            u_copy(n, dev, False, gp_send.at[n, mask], gp_recv.at[n, mask], partner).wait_recv()
    for cp in sent:
        cp.wait_send()
    for cp in local:
        cp.wait()
    for j in range(3):
        vcopy(my_strip, j, v_send, v_recv, far).wait_send()
        vcopy(my_strip, j, v_pair_send, v_pair_recv, partner).wait_send()
        vcopy(far_strip, j, v_fwd_send, v_fwd_recv, partner).wait_send()
    for p in range(N_PROD - SLOTS, N_PROD):
        drain(p)


def tail(u_ref, a_old, a_sum, s_old, s_sum, u_out, a_new, s_new):
    scale = (1.0 - FACTOR_DECAY) / (ROWS * 16)
    u_out[:, :D - WIDE] = u_ref[:, :D - WIDE].astype(F32)
    u_out[:, D - WIDE:] = u_ref[:, D - WIDE:D].astype(F32) + u_ref[:, D:].astype(F32)
    a_new[...] = FACTOR_DECAY * a_old[...] + scale * a_sum[...]
    s_new[...] = FACTOR_DECAY * s_old[...] + scale * s_sum[...]


def solution(mesh):
    dma = pltpu.SemaphoreType.DMA
    any_spec = pl.BlockSpec(memory_space=pl.ANY)
    vmem_spec = pl.BlockSpec(memory_space=pltpu.VMEM)

    def device_step(x_loc, dy_loc, weights, a_old_rows, s_old_rows, a_inv_rows, s_inv):
        u_parts, a_sum, s_sum = pl.pallas_call(
            kernel,
            out_shape=(
                jax.ShapeDtypeStruct((N_LAYERS * D, D + WIDE), BF16),
                jax.ShapeDtypeStruct((STRIP, D), F32),
                jax.ShapeDtypeStruct((STRIP, D), F32),
            ),
            in_specs=[any_spec] * 5,
            out_specs=(any_spec, vmem_spec, vmem_spec),
            scratch_shapes=[
                pltpu.VMEM((8, ROWS, D), BF16),
                pltpu.VMEM((N_LAYERS, D, D), BF16),
                pltpu.VMEM((2, D, D), F32),
                pltpu.VMEM((PAIR_SLOTS, 2, STRIP, D), F32),
                pltpu.VMEM((SLOTS, 2, STRIP, D), F32),
                pltpu.VMEM((EARLY, 2, STRIP, D), BF16),
                pltpu.VMEM((3, 7, STRIP, CHUNK), F32),
                pltpu.VMEM((2, 3, 4, STRIP, CHUNK), BF16),
                pltpu.VMEM((2, 3, 3, STRIP, CHUNK), F32),
                pltpu.VMEM((STRIP, D), F32),
                pltpu.VMEM((D, D), F32),
                pltpu.VMEM((STRIP, D), F32),
                pltpu.VMEM((D, D), F32),
                pltpu.VMEM((STRIP, D + WIDE), BF16),
                dma((5,)), dma((2, 2)), dma((PAIR_SLOTS, 2)), pltpu.SemaphoreType.REGULAR,
                dma((SLOTS, 3, 2)), dma((3, 3, 7)),
                dma((3,)), dma((3,)), dma((3,)), dma((3,)), dma((3,)), dma((3,)),
                dma((4, 8)), dma((4, 8)), dma((4, 8)), dma((4, 8)), dma((4,)),
            ],
            compiler_params=pltpu.CompilerParams(
                collective_id=0, has_side_effects=True, vmem_limit_bytes=67043328),
        )(x_loc, dy_loc, weights, a_inv_rows, s_inv)
        u_block = pl.BlockSpec((N_LAYERS * D // TAIL_STEPS, D + WIDE), lambda i: (i, 0))
        out_block = pl.BlockSpec((N_LAYERS * D // TAIL_STEPS, D), lambda i: (i, 0))
        row_block = pl.BlockSpec((STRIP // TAIL_STEPS, D), lambda i: (i, 0))
        u_flat, a_new, s_new = pl.pallas_call(
            tail,
            grid=(TAIL_STEPS,),
            out_shape=(
                jax.ShapeDtypeStruct((N_LAYERS * D, D), F32),
                jax.ShapeDtypeStruct((STRIP, D), F32),
                jax.ShapeDtypeStruct((STRIP, D), F32),
            ),
            in_specs=[u_block] + [row_block] * 4,
            out_specs=(out_block, row_block, row_block),
        )(u_parts, a_old_rows, a_sum, s_old_rows, s_sum)
        return u_flat.reshape(N_LAYERS, D, D), a_new, s_new

    row_spec = P("data", None)
    return jax.shard_map(
        device_step,
        mesh=mesh,
        in_specs=(row_spec, row_spec, P(), row_spec, row_spec, row_spec, P()),
        out_specs=(P(), row_spec, row_spec),
        check_vma=False,
    )
```

```python
import jax
import jax.numpy as jnp
from jax import lax
from jax.experimental import pallas as pl
from jax.experimental.pallas import tpu as pltpu
from jax.sharding import PartitionSpec as P

FACTOR_DECAY = 0.75
MESH = pl.DeviceIdType.MESH
F32 = jnp.float32
BF16 = jnp.bfloat16
N_LAYERS = 4
D = 768
STRIP = 192
ROWS = 2048
BLOCK = 512
CHUNK = 256
MBLOCK = 384
PAIR_SLOTS = 2
TAIL_STEPS = 4
SLOTS = 7
GELU_C = 0.7978845608028654
GELU_K = 0.044715
CONTRACT_ROWS = (((0,), (0,)), ((), ()))
SCHEDULE = [
    "F0 F1 P0.0 P0.1", "R0 F2 R1 P2.3", "S0.1.0 S0.1.1 S0.1.2 B3", "R2 S1.1.0 S1.1.1 S1.1.2",
    "P2.2 S0.2.0 S0.2.2 B2", "R3 S2.1.0 S0.2.1 P2.1", "S2.1.1 S2.1.2 S0.3.0 S0.3.2", "S1.2.1 S1.2.2 B1 R4",
    "S3.1.0 S1.2.0 P2.0 S2.2.0", "S2.2.2 S3.1.1 S3.1.2 S0.3.1", "S1.3.1 P1.2 R5 S3.2.0", "S4.1.0 S1.3.2 P0.3 R6",
    "S2.2.1 S3.2.2 S4.1.2 P1.3", "R7 S3.2.1 S4.1.1 S1.3.0", "P1.1 R8 S2.3.0 S2.3.2", "S5.1.0 S5.1.1 S6.1.0 P1.0",
    "S2.3.1 R9 S3.3.0 S4.2.0", "S4.2.2 S6.1.1 P0.2 S3.3.1", "S5.1.2 S6.1.2 S7.1.0 S7.1.1",
    "S8.1.0 S3.3.2 R10 S7.1.2", "S8.1.1 S9.1.0 S5.2.1 S5.2.0", "S8.1.2 S6.2.0 S6.2.2 S9.1.1",
    "S4.2.1 S5.2.2 S10.1.0 S4.3.2", "S9.1.2 S4.3.1 S4.3.0 R11", "S7.2.0 S7.2.1 S7.2.2 S10.1.1",
    "S6.2.1 S5.3.1 S5.3.2 S5.3.0", "V S9.2.2 S8.2.0 S10.1.2", "S6.3.2 S6.3.0 S8.2.2 S11.1.0",
    "S8.2.1 S10.2.0 S6.3.1 S11.1.1", "S10.2.1 S9.2.0 S7.3.2 S7.3.1", "S11.1.2 S8.3.2 S7.3.0 W0",
    "U0 S11.2.0 S9.3.2 S9.2.1", "W1 S8.3.0 S11.2.1 S10.3.0", "U1 f0.2 S9.3.0 W2", "U2 f0.4 f1.2 S11.3.0",
    "S8.3.1 S10.2.2 f1.4 S10.3.1", "f0.6 f2.4 S9.3.1 f3.4", "S11.3.1 S10.3.2 f2.2 f3.2", "S11.2.2 f0.1 f1.1 f1.6",
    "f3.6 f2.1 S11.3.2 f3.1", "f0.3 f2.6 f2.5 f3.5", "f1.3 f3.3 f0.5 f2.3", "f3.7 f1.5 f2.7 f0.7", "f1.7",
]
EVENTS = [(e[0], [int(a) for a in e[1:].split(".") if a]) for group in SCHEDULE for e in group.split()]
PRODUCTS = [tuple(args) for what, args in EVENTS if what == "P"]
N_PROD = len(PRODUCTS)
EARLY = 2
FIRST_LATE = 5
ORDERS = [(1, 2, 4), (2, 4, 1), (4, 1, 2)]
WIDE = 128
PIECES = [(0, 256, (1, 2, 4)), (256, 256, (1, 2, 4)), (512, 256, (2, 4, 1)), (768, 128, (4, 1, 2))]


def xor_chip(chip, mask):
    out = chip
    for bit in (1, 2, 4):
        if mask & bit:
            out = out + bit - 2 * bit * lax.rem(lax.div(chip, bit), 2)
    return out


def unit(j, step, layer, tx):
    bits = {1: tx, 2: layer % 2, 4: layer // 2}
    index = (0, 4, 6)[step]
    for place, dim in enumerate(ORDERS[j][step + 1:]):
        index = index + bits[dim] * (place + 1)
    return index


def cols(j):
    return pl.ds(j * CHUNK, CHUNK)


def kernel(x_hbm, dy_hbm, w_hbm, ainv_hbm, sinv_hbm, u_hbm, a_out, s_out,
           act, wts, part, pair_buf, acc, stg, recv_g, recv_as, recv_late, gsum, sinv, ainv, vfull, ustrip,
           load_sem, pair_send, pair_recv, credit, send_sem, recv_sem,
           v_send, v_recv, v_fwd_send, v_fwd_recv, v_pair_send, v_pair_recv,
           g_send, g_recv, gp_send, gp_recv, loc_sem):
    me = lax.axis_index("data")
    core = lax.rem(me, 2)
    chip = lax.div(me, 2)
    xbit = lax.rem(chip, 2)
    ybit = lax.rem(lax.div(chip, 2), 2)
    zbit = lax.div(chip, 4)
    layer_own = lax.div(chip, 2)
    partner = chip * 2 + 1 - core

    def peer(mask):
        return xor_chip(chip, mask) * 2 + core

    loads = [
        pltpu.make_async_copy(x_hbm, act.at[0], load_sem.at[0]),
        pltpu.make_async_copy(w_hbm, wts, load_sem.at[1]),
        pltpu.make_async_copy(dy_hbm, act.at[7], load_sem.at[2]),
        pltpu.make_async_copy(ainv_hbm, ainv, load_sem.at[3]),
        pltpu.make_async_copy(sinv_hbm.at[layer_own], sinv, load_sem.at[4]),
    ]
    for ld in loads:
        ld.start()

    barrier = pltpu.get_barrier_semaphore()
    pl.semaphore_signal(barrier, inc=1, device_id=(partner,), device_id_type=MESH)
    for mask in (1, 2, 4):
        pl.semaphore_signal(barrier, inc=1, device_id=(peer(mask),), device_id_type=MESH)
    pl.semaphore_wait(barrier, 4)


    def pair_copy(p, tx):
        row = pl.multiple_of((2 * tx + 1 - core) * STRIP, STRIP)
        return pltpu.make_async_remote_copy(
            src_ref=part.at[p % 2, pl.ds(row, STRIP)],
            dst_ref=pair_buf.at[p % PAIR_SLOTS, tx],
            send_sem=pair_send.at[p % 2, tx],
            recv_sem=pair_recv.at[p % PAIR_SLOTS, tx],
            device_id=(partner,),
            device_id_type=MESH,
        )

    def landing(kind, j, u, step):
        if kind != 2 and step > 0:
            return recv_late.at[kind, j, u - 4]
        return recv_g.at[j, u] if kind == 2 else recv_as.at[kind, j, u]

    def staged(p, tx, j):
        if p < FIRST_LATE:
            return stg, (sum(k != 2 for k, _ in PRODUCTS[:p]), tx, slice(None), cols(j))
        n = sum(k != 2 for k, _ in PRODUCTS[FIRST_LATE:p])
        return wts, (n // 2, pl.ds((n % 2) * 2 * STRIP + tx * STRIP, STRIP), cols(j))

    def strip_copy(p, j, step, tx):
        kind, layer = PRODUCTS[p]
        u = unit(j, step, layer, tx)
        if kind == 2 or step > 0:
            src = acc.at[p % SLOTS, tx, :, cols(j)]
        else:
            ref, idx = staged(p, tx, j)
            src = ref.at[idx]
        return pltpu.make_async_remote_copy(
            src_ref=src,
            dst_ref=landing(kind, j, u, step),
            send_sem=send_sem.at[p % SLOTS, j, tx],
            recv_sem=recv_sem.at[kind, j, u],
            device_id=(peer(ORDERS[j][step]),),
            device_id_type=MESH,
        )

    def product(p):
        kind, layer = PRODUCTS[p]
        left = layer if kind != 1 else 4 + layer
        right = layer if kind == 0 else 4 + layer

        def body(mb, carry):
            ms = pl.ds(pl.multiple_of(mb * MBLOCK, MBLOCK), MBLOCK)
            part[p % 2, ms] = lax.dot_general(act[left, :, ms], act[right], CONTRACT_ROWS,
                                              preferred_element_type=F32)
            return carry
        lax.fori_loop(0, D // MBLOCK, body, 0)
        if p >= PAIR_SLOTS:
            pl.semaphore_wait(credit, 1)
        for tx in range(2):
            pair_copy(p, tx).start()

    def equal(dim, layer):
        z_l, y_l = divmod(layer, 2)
        return ybit == y_l if dim == 2 else zbit == z_l

    def drain(p):
        _, layer = PRODUCTS[p]
        for j in range(3):
            for step, dim in enumerate(ORDERS[j]):
                before = ORDERS[j][:step]
                sent_here = chip >= 0
                for other in before:
                    if other != 1:
                        sent_here = jnp.logical_and(sent_here, equal(other, layer))
                strips = [xbit] if 1 in before else [0, 1]
                if dim == 1:
                    strips = [1 - xbit]
                else:
                    sent_here = jnp.logical_and(sent_here, jnp.logical_not(equal(dim, layer)))

                @pl.when(sent_here)
                def _(j=j, step=step, strips=strips):
                    for tx in strips:
                        strip_copy(p, j, step, tx).wait_send()

    def stage(p, step, chunks=(0, 1, 2)):
        kind, layer = PRODUCTS[p]
        slot = p % SLOTS
        for j in chunks:
            order = ORDERS[j]
            before = order[:step]
            active = None
            for dim in before:
                if dim != 1:
                    cond = equal(dim, layer)
                    active = cond if active is None else jnp.logical_and(active, cond)
            strips = [xbit] if 1 in before else [0, 1]

            def body(j=j, order=order, strips=strips):
                if step > 0:
                    for tx in strips:
                        strip_copy(p, j, step - 1, tx).wait_recv()
                        u = unit(j, step - 1, layer, tx)
                        got = landing(kind, j, u, step - 1)[...].astype(F32)
                        new = acc[slot, tx, :, cols(j)] + got
                        if step < 3:
                            acc[slot, tx, :, cols(j)] = new
                if step == 3:
                    if kind == 2:
                        gsum[:, cols(j)] = new * (1.0 / (ROWS * 16))
                    elif kind == 0:
                        a_out[:, cols(j)] = new
                    else:
                        s_out[:, cols(j)] = new
                    return
                dim = order[step]
                if dim == 1:
                    strip_copy(p, j, step, 1 - xbit).start()
                else:
                    @pl.when(jnp.logical_not(equal(dim, layer)))
                    def _():
                        for tx in strips:
                            strip_copy(p, j, step, tx).start()

            if active is None:
                body()
            else:
                pl.when(active)(body)
    def pair_sum(p):
        kind, layer = PRODUCTS[p]
        slot = p % SLOTS
        if p >= SLOTS:
            drain(p - SLOTS)
        for tx in range(2):
            pair_copy(p, tx).wait_recv()
            row = pl.multiple_of((2 * tx + core) * STRIP, STRIP)
            total = part[p % 2, pl.ds(row, STRIP)] + pair_buf[p % PAIR_SLOTS, tx]
            acc[slot, tx] = total
            if kind != 2:
                for j in range(3):
                    ref, idx = staged(p, tx, j)
                    ref[idx] = total[:, j * CHUNK:(j + 1) * CHUNK].astype(BF16)
        stage(p, 0)
        for tx in range(2):
            pair_copy(p, tx).wait_send()
        if p + PAIR_SLOTS < N_PROD:
            pl.semaphore_signal(credit, inc=1, device_id=(partner,), device_id_type=MESH)


    def forward(layer):
        def body(rb, carry):
            rows = pl.ds(pl.multiple_of(rb * BLOCK, BLOCK), BLOCK)
            z = jnp.dot(act[layer, rows], wts[layer], preferred_element_type=F32).astype(BF16)
            act[4 + layer, rows] = z
            zf = z.astype(F32)
            half = 0.5 * zf
            t = jnp.tanh(zf * (GELU_C + (GELU_C * GELU_K) * (zf * zf)))
            act[layer + 1, rows] = (half + half * t).astype(BF16)
            return carry
        lax.fori_loop(0, ROWS // BLOCK, body, 0)

    def backward(layer):
        def body(rb, carry):
            rows = pl.ds(pl.multiple_of(rb * BLOCK, BLOCK), BLOCK)
            d_act = lax.dot_general(act[4 + layer, rows], wts[layer], (((1,), (1,)), ((), ())),
                                    preferred_element_type=F32).astype(BF16).astype(F32)
            z = act[3 + layer, rows].astype(F32)
            z2 = z * z
            t = jnp.tanh(z * (GELU_C + (GELU_C * GELU_K) * z2))
            slope = (0.5 + 0.5 * t) + (0.5 * z) * ((1.0 - t * t) * (GELU_C + (3.0 * GELU_C * GELU_K) * z2))
            act[3 + layer, rows] = (d_act * slope).astype(BF16)
            return carry
        lax.fori_loop(0, ROWS // BLOCK, body, 0)


    my_strip = 2 * xbit + core
    pair_strip = 2 * xbit + 1 - core
    far_strip = 2 * (1 - xbit) + core
    far_pair_strip = 2 * (1 - xbit) + 1 - core
    far = peer(1)

    def vblock(strip, j):
        return vfull.at[pl.ds(pl.multiple_of(strip * STRIP, STRIP), STRIP), cols(j)]

    def vcopy(strip, j, ssem, rsem, dev):
        return pltpu.make_async_remote_copy(
            src_ref=vblock(strip, j), dst_ref=vblock(strip, j), send_sem=ssem.at[j], recv_sem=rsem.at[j],
            device_id=(dev,), device_id_type=MESH)

    def v_stage():
        loads[3].wait()
        loads[4].wait()
        for j in range(3):
            vfull[pl.ds(pl.multiple_of(my_strip * STRIP, STRIP), STRIP), cols(j)] = jnp.dot(
                gsum[...], sinv[:, cols(j)], precision=lax.Precision.HIGHEST, preferred_element_type=F32)
            vcopy(my_strip, j, v_send, v_recv, far).start()
            vcopy(my_strip, j, v_pair_send, v_pair_recv, partner).start()

    def u_block(dev, n):
        first, width, _ = PIECES[n]
        return u_hbm.at[pl.ds(pl.multiple_of(dev * STRIP, STRIP), STRIP), pl.ds(first, width)]

    def u_own(n):
        first, width, _ = PIECES[n]
        return ustrip.at[:, pl.ds(first, width)]

    def u_copy(n, dev, src_own, ssem, rsem, target):
        return pltpu.make_async_remote_copy(
            src_ref=u_own(n) if src_own else u_block(dev, n), dst_ref=u_block(dev, n), send_sem=ssem, recv_sem=rsem,
            device_id=(target,), device_id_type=MESH)

    sent = []

    def launch(n, mask, dims):
        dev = peer(mask) if mask else me
        for d in dims:
            m = mask | d
            cp = u_copy(n, dev, mask == 0, g_send.at[n, m], g_recv.at[n, m], peer(d))
            cp.start()
            sent.append(cp)
        cp = u_copy(n, dev, mask == 0, gp_send.at[n, mask], gp_recv.at[n, mask], partner)
        cp.start()
        sent.append(cp)

    local = [pltpu.make_async_copy(u_own(n), u_block(me, n), loc_sem.at[n]) for n in range(4)]

    def v_pass(j):
        vcopy(far_strip, j, v_send, v_recv, far).wait_recv()
        vcopy(far_strip, j, v_fwd_send, v_fwd_recv, partner).start()

    def u_stage(j):
        vcopy(pair_strip, j, v_pair_send, v_pair_recv, partner).wait_recv()
        vcopy(far_pair_strip, j, v_fwd_send, v_fwd_recv, partner).wait_recv()
        u_rows = jnp.dot(ainv[...], vfull[:, cols(j)], precision=lax.Precision.HIGHEST, preferred_element_type=F32)
        high = u_rows.astype(BF16)
        ustrip[:, cols(j)] = high
        pieces = [j]
        if j == 2:
            ustrip[:, D:] = (u_rows - high.astype(F32))[:, CHUNK - WIDE:].astype(BF16)
            pieces = [2, 3]
        for n in pieces:
            launch(n, 0, PIECES[n][2])
            local[n].start()

    def u_forward(n, mask):
        order = PIECES[n][2]
        last = max(i for i in range(3) if mask & order[i])
        u_copy(n, peer(mask), False, g_send.at[n, mask], g_recv.at[n, mask], peer(order[last])).wait_recv()
        launch(n, mask, order[last + 1:])


    waited = set()

    def loaded(n):
        if n not in waited:
            waited.add(n)
            loads[n].wait()

    loaded(0)
    n_prod = 0
    for what, args in EVENTS:
        if what == "P":
            if args[0] == 1 or (args[0] == 2 and args[1] == 3):
                loaded(2)
            product(n_prod)
            n_prod += 1
        elif what == "R":
            pair_sum(args[0])
        elif what == "S":
            stage(args[0], args[1], (args[2],))
        elif what == "F":
            loaded(1)
            forward(args[0])
        elif what == "B":
            loaded(2)
            backward(args[0])
        elif what == "V":
            v_stage()
        elif what == "U":
            u_stage(args[0])
        elif what == "W":
            v_pass(args[0])
        else:
            u_forward(*args)
    for n in range(4):
        for mask in range(8):
            dev = xor_chip(chip, mask) * 2 + 1 - core
            u_copy(n, dev, False, gp_send.at[n, mask], gp_recv.at[n, mask], partner).wait_recv()
    for cp in sent:
        cp.wait_send()
    for cp in local:
        cp.wait()
    for j in range(3):
        vcopy(my_strip, j, v_send, v_recv, far).wait_send()
        vcopy(my_strip, j, v_pair_send, v_pair_recv, partner).wait_send()
        vcopy(far_strip, j, v_fwd_send, v_fwd_recv, partner).wait_send()
    for p in range(N_PROD - SLOTS, N_PROD):
        drain(p)


def tail(u_ref, a_old, a_sum, s_old, s_sum, u_out, a_new, s_new):
    scale = (1.0 - FACTOR_DECAY) / (ROWS * 16)
    u_out[:, :D - WIDE] = u_ref[:, :D - WIDE].astype(F32)
    u_out[:, D - WIDE:] = u_ref[:, D - WIDE:D].astype(F32) + u_ref[:, D:].astype(F32)
    a_new[...] = FACTOR_DECAY * a_old[...] + scale * a_sum[...]
    s_new[...] = FACTOR_DECAY * s_old[...] + scale * s_sum[...]


def solution(mesh):
    dma = pltpu.SemaphoreType.DMA
    any_spec = pl.BlockSpec(memory_space=pl.ANY)
    vmem_spec = pl.BlockSpec(memory_space=pltpu.VMEM)

    def device_step(x_loc, dy_loc, weights, a_old_rows, s_old_rows, a_inv_rows, s_inv):
        u_parts, a_sum, s_sum = pl.pallas_call(
            kernel,
            out_shape=(
                jax.ShapeDtypeStruct((N_LAYERS * D, D + WIDE), BF16),
                jax.ShapeDtypeStruct((STRIP, D), F32),
                jax.ShapeDtypeStruct((STRIP, D), F32),
            ),
            in_specs=[any_spec] * 5,
            out_specs=(any_spec, vmem_spec, vmem_spec),
            scratch_shapes=[
                pltpu.VMEM((8, ROWS, D), BF16),
                pltpu.VMEM((N_LAYERS, D, D), BF16),
                pltpu.VMEM((2, D, D), F32),
                pltpu.VMEM((PAIR_SLOTS, 2, STRIP, D), F32),
                pltpu.VMEM((SLOTS, 2, STRIP, D), F32),
                pltpu.VMEM((EARLY, 2, STRIP, D), BF16),
                pltpu.VMEM((3, 7, STRIP, CHUNK), F32),
                pltpu.VMEM((2, 3, 4, STRIP, CHUNK), BF16),
                pltpu.VMEM((2, 3, 3, STRIP, CHUNK), F32),
                pltpu.VMEM((STRIP, D), F32),
                pltpu.VMEM((D, D), F32),
                pltpu.VMEM((STRIP, D), F32),
                pltpu.VMEM((D, D), F32),
                pltpu.VMEM((STRIP, D + WIDE), BF16),
                dma((5,)), dma((2, 2)), dma((PAIR_SLOTS, 2)), pltpu.SemaphoreType.REGULAR,
                dma((SLOTS, 3, 2)), dma((3, 3, 7)),
                dma((3,)), dma((3,)), dma((3,)), dma((3,)), dma((3,)), dma((3,)),
                dma((4, 8)), dma((4, 8)), dma((4, 8)), dma((4, 8)), dma((4,)),
            ],
            compiler_params=pltpu.CompilerParams(
                collective_id=0, has_side_effects=True, vmem_limit_bytes=67043328),
        )(x_loc, dy_loc, weights, a_inv_rows, s_inv)
        u_block = pl.BlockSpec((N_LAYERS * D // TAIL_STEPS, D + WIDE), lambda i: (i, 0))
        out_block = pl.BlockSpec((N_LAYERS * D // TAIL_STEPS, D), lambda i: (i, 0))
        row_block = pl.BlockSpec((STRIP // TAIL_STEPS, D), lambda i: (i, 0))
        u_flat, a_new, s_new = pl.pallas_call(
            tail,
            grid=(TAIL_STEPS,),
            out_shape=(
                jax.ShapeDtypeStruct((N_LAYERS * D, D), F32),
                jax.ShapeDtypeStruct((STRIP, D), F32),
                jax.ShapeDtypeStruct((STRIP, D), F32),
            ),
            in_specs=[u_block] + [row_block] * 4,
            out_specs=(out_block, row_block, row_block),
        )(u_parts, a_old_rows, a_sum, s_old_rows, s_sum)
        return u_flat.reshape(N_LAYERS, D, D), a_new, s_new

    row_spec = P("data", None)
    return jax.shard_map(
        device_step,
        mesh=mesh,
        in_specs=(row_spec, row_spec, P(), row_spec, row_spec, row_spec, P()),
        out_specs=(P(), row_spec, row_spec),
        check_vma=False,
    )
```
